8 devices in a mesh: data: 2 (over z, y), seq: 4 (over x, core).
Axes of the slice: x: 2, y: 2, z: 1, core: 2. Of those that a mesh axis runs over, the one named last changes fastest.
Arguments:
- act_in: bfloat16 [128, 576, 768], P('data', 'seq'), parts along dimension 0
- grad_out: bfloat16 [128, 576, 768], P('data', 'seq'), parts along dimension 0
- ln1_scale: float32 [768], replicated
- ln1_shift: float32 [768], replicated
- w_tok1: bfloat16 [576, 384], replicated
- b_tok1: float32 [384], replicated
- w_tok2: bfloat16 [384, 576], replicated
- b_tok2: float32 [576], replicated
- ln2_scale: float32 [768], replicated
- ln2_shift: float32 [768], replicated
- w_chan1: bfloat16 [768, 3072], replicated
- b_chan1: float32 [3072], replicated
- w_chan2: bfloat16 [3072, 768], replicated
- b_chan2: float32 [768], replicated
Outputs:
- output 1: bfloat16 [128, 576, 768], P('data', 'seq'), parts along dimension 0
- output 2: bfloat16 [128, 576, 768], P('data', 'seq'), parts along dimension 0
- output 3: float32 [1152, 384], P('data'), parts along dimension 0
- output 4: float32 [768, 576], P('data'), parts along dimension 0
- output 5: float32 [1536, 3072], P('data'), parts along dimension 0
- output 6: float32 [6144, 768], P('data'), parts along dimension 0
There are 2 independent parts. The reference program is written for one: setup_inputs(seed, part) draws one part's arguments, and reference() takes and returns one part's arrays. A program takes and returns all parts, laid end to end along the dimension named above; an argument that names none is the same for every part.
All inputs are finite; a program needn't handle non-finite values.
Results may differ from the reference program's by a relative error of at most 0.0166067.
Values are sent between devices in bfloat16 or wider.
A program may use at most 1 GiB of HBM per device.

```python
import jax
import jax.numpy as jnp
from jax import lax

IMAGES = 64
PATCHES = 576
CHANNELS = 768
TOKEN_HID = 384
CHAN_HID = 3072

LN_EPS = 1e-6


def setup_inputs(seed: int = 0, part: int = 0) -> dict:
    part_key = jax.random.fold_in(jax.random.key(seed), part)
    act_key, grad_key = jax.random.split(part_key)
    weight_keys = jax.random.split(jax.random.key(seed + 1), 12)

    def draw_normal(key_index, shape, spread):
        return jax.random.normal(weight_keys[key_index], shape, jnp.float32) * spread

    act_in = jax.random.normal(act_key, (IMAGES, PATCHES, CHANNELS), jnp.float32)
    grad_out = jax.random.normal(grad_key, (IMAGES, PATCHES, CHANNELS), jnp.float32)
    return {
        "act_in": act_in.astype(jnp.bfloat16),
        "grad_out": grad_out.astype(jnp.bfloat16),
        "ln1_scale": 1.0 + draw_normal(0, (CHANNELS,), 0.3),
        "ln1_shift": draw_normal(1, (CHANNELS,), 0.3),
        "w_tok1": draw_normal(2, (PATCHES, TOKEN_HID), PATCHES ** -0.5).astype(jnp.bfloat16),
        "b_tok1": draw_normal(3, (TOKEN_HID,), 0.5),
        "w_tok2": draw_normal(4, (TOKEN_HID, PATCHES), TOKEN_HID ** -0.5).astype(jnp.bfloat16),
        "b_tok2": draw_normal(5, (PATCHES,), 0.5),
        "ln2_scale": 1.0 + draw_normal(6, (CHANNELS,), 0.3),
        "ln2_shift": draw_normal(7, (CHANNELS,), 0.3),
        "w_chan1": draw_normal(8, (CHANNELS, CHAN_HID), CHANNELS ** -0.5).astype(jnp.bfloat16),
        "b_chan1": draw_normal(9, (CHAN_HID,), 0.5),
        "w_chan2": draw_normal(10, (CHAN_HID, CHANNELS), CHAN_HID ** -0.5).astype(jnp.bfloat16),
        "b_chan2": draw_normal(11, (CHANNELS,), 0.5),
    }


def layer_norm(rows_in, ln_scale, ln_shift):
    widened = rows_in.astype(jnp.float32)
    row_mean = jnp.mean(widened, axis=-1, keepdims=True)
    centered = widened - row_mean
    row_var = jnp.mean(centered * centered, axis=-1, keepdims=True)
    return (centered * lax.rsqrt(row_var + LN_EPS) * ln_scale + ln_shift).astype(jnp.bfloat16)


def gelu_bf16(pre_act):
    return jax.nn.gelu(pre_act.astype(jnp.float32)).astype(jnp.bfloat16)


def reference(act_in, grad_out, ln1_scale, ln1_shift, w_tok1, b_tok1, w_tok2, b_tok2,
              ln2_scale, ln2_shift, w_chan1, b_chan1, w_chan2, b_chan2):
    def layer_forward(tok1_wide, tok2_wide, chan1_wide, chan2_wide, image):
        normed = layer_norm(image, ln1_scale, ln1_shift)
        tok_pre = (jnp.einsum("sd,sc->dc", tok1_wide, normed.astype(jnp.float32))
                   + b_tok1[:, None]).astype(jnp.bfloat16)
        tok_act = gelu_bf16(tok_pre)
        tok_out = (jnp.einsum("ds,dc->sc", tok2_wide, tok_act.astype(jnp.float32))
                   + b_tok2[:, None]).astype(jnp.bfloat16)
        mid_act = (image.astype(jnp.float32) + tok_out.astype(jnp.float32)).astype(jnp.bfloat16)
        normed_mid = layer_norm(mid_act, ln2_scale, ln2_shift)
        chan_pre = (jnp.einsum("sc,ch->sh", normed_mid.astype(jnp.float32), chan1_wide)
                    + b_chan1).astype(jnp.bfloat16)
        chan_act = gelu_bf16(chan_pre)
        chan_out = jnp.einsum("sh,hc->sc", chan_act.astype(jnp.float32), chan2_wide) + b_chan2
        return (mid_act.astype(jnp.float32) + chan_out).astype(jnp.bfloat16)

    tok1_wide = w_tok1.astype(jnp.float32)
    tok2_wide = w_tok2.astype(jnp.float32)
    chan1_wide = w_chan1.astype(jnp.float32)
    chan2_wide = w_chan2.astype(jnp.float32)

    def image_step(grad_sums, image_pair):
        image, image_grad = image_pair
        image_out, pullback = jax.vjp(layer_forward, tok1_wide, tok2_wide, chan1_wide, chan2_wide, image)
        cotangents = pullback(image_grad)
        new_sums = tuple(total + piece for total, piece in zip(grad_sums, cotangents[:4]))
        return new_sums, (image_out, cotangents[4])

    zero_sums = (jnp.zeros(w_tok1.shape, jnp.float32), jnp.zeros(w_tok2.shape, jnp.float32),
                 jnp.zeros(w_chan1.shape, jnp.float32), jnp.zeros(w_chan2.shape, jnp.float32))
    weight_sums, (act_out, grad_in) = lax.scan(image_step, zero_sums, (act_in, grad_out))
    return act_out, grad_in, weight_sums[0], weight_sums[1], weight_sums[2], weight_sums[3]
```

```python
import functools

import jax
import jax.numpy as jnp
from jax import lax
from jax.experimental import pallas as pl
from jax.experimental.pallas import tpu as pltpu
from jax.sharding import PartitionSpec as P


LN_EPS = 1e-6
GELU_C = 0.7978845608028654
GELU_K = 0.044715
F32 = jnp.float32
BF16 = jnp.bfloat16

CHUNK_SIZES = (2, 4, 4, 4, 2)
PIECES = 3
HID_BLOCK = 512
ROW_BLOCK = 48
COL_BLOCK = 256


def gelu_parts(pre):
    sq = pre * pre
    th = jnp.tanh(pre * (GELU_C + (GELU_C * GELU_K) * sq))
    half = 0.5 * pre
    cdf = 0.5 + 0.5 * th
    slope = cdf + (half * (1.0 - th * th)) * (GELU_C + (3.0 * GELU_C * GELU_K) * sq)
    return pre * cdf, slope


def gelu_value(pre):
    sq = pre * pre
    th = jnp.tanh(pre * (GELU_C + (GELU_C * GELU_K) * sq))
    return pre * (0.5 + 0.5 * th)


def gelu_slope(pre):
    return gelu_parts(pre)[1]


def dot(a, b):
    return jnp.dot(a, b, preferred_element_type=F32)


def dot_nt(a, b):
    return lax.dot_general(a, b, (((1,), (1,)), ((), ())), preferred_element_type=F32)


def layer_kernel(first, *refs):
    x_refs, dz_refs = refs[0:4], refs[4:8]
    (ln1_s, ln1_b, ln2_s, ln2_b, b_c1, b_c2, b_t1, b_t2, w_t1, w_t1t, w_t2, w_t2t,
     w_c1, w_c2) = refs[8:22]
    pos = 22
    if not first:
        acc_in = refs[pos:pos + 4]
        pos += 4
    z_refs, dx_refs = refs[pos:pos + 4], refs[pos + 4:pos + 8]
    acc_out = refs[pos + 8:pos + 12]
    (g_c1, g_c2, g_t1, g_t2, u_s, v_s, vt_s, dz_s, h_s, g_s, x1_s, dv_s, acc_s, sem) = refs[pos + 12:]
    accs = (g_t1, g_t2, g_c1, g_c2)
    step = pl.program_id(0)
    rows = x_refs[0].shape[1]
    total_rows = 4 * rows
    chans = u_s.shape[1]
    hid = w_c1.shape[1]

    @pl.when(step == 0)
    def _():
        if first:
            for acc in accs:
                acc[...] = jnp.zeros_like(acc)
        else:
            copies = [pltpu.make_async_copy(src, acc, sem.at[i])
                      for i, (src, acc) in enumerate(zip(acc_in, accs))]
            for cp in copies:
                cp.start()
            for cp in copies:
                cp.wait()

    def norm(val, scale, shift):
        mean = jnp.mean(val, axis=-1, keepdims=True)
        cen = val - mean
        var = jnp.mean(cen * cen, axis=-1, keepdims=True)
        return (cen * lax.rsqrt(var + LN_EPS) * scale + shift).astype(BF16)

    def norm_grad(val, grad, scale):
        mean = jnp.mean(val, axis=-1, keepdims=True)
        cen = val - mean
        var = jnp.mean(cen * cen, axis=-1, keepdims=True)
        inv = lax.rsqrt(var + LN_EPS)
        hat = cen * inv
        gs = grad * scale
        m1 = jnp.mean(gs, axis=-1, keepdims=True)
        m2 = jnp.mean(gs * hat, axis=-1, keepdims=True)
        return (inv * (gs - m1 - hat * m2)).astype(BF16)

    per_block = rows // ROW_BLOCK

    for k in range(4):
        def ln1_step(i, carry, k=k):
            r = pl.multiple_of(i * ROW_BLOCK, 16)
            dst = pl.ds(k * rows + r, ROW_BLOCK)
            u_s[dst, :] = norm(x_refs[k][0, pl.ds(r, ROW_BLOCK), :].astype(F32), ln1_s[...], ln1_b[...])
            dz_s[dst, :] = dz_refs[k][0, pl.ds(r, ROW_BLOCK), :]
            return carry

        lax.fori_loop(0, per_block, ln1_step, 0, unroll=True)

    for n in range(chans // COL_BLOCK):
        cols = slice(n * COL_BLOCK, (n + 1) * COL_BLOCK)
        h = (dot(w_t1t[...], u_s[:, cols]) + b_t1[...]).astype(BF16)
        h_s[:, cols] = h
        g = gelu_value(h.astype(F32)).astype(BF16)
        g_s[:, cols] = g
        t = (dot(w_t2t[...], g) + b_t2[...]).astype(BF16)
        for k in range(4):
            part = slice(k * rows, (k + 1) * rows)
            x1_s[part, cols] = (x_refs[k][0, :, cols].astype(F32) + t[part].astype(F32)).astype(BF16)

    def ln2_step(i, carry):
        r = pl.ds(pl.multiple_of(i * ROW_BLOCK, 16), ROW_BLOCK)
        v_s[r, :] = norm(x1_s[r, :].astype(F32), ln2_s[...], ln2_b[...])
        return carry

    lax.fori_loop(0, total_rows // ROW_BLOCK, ln2_step, 0, unroll=True)

    vt_s[...] = v_s[...].T
    acc_s[...] = jnp.zeros_like(acc_s)
    dv_s[...] = jnp.zeros_like(dv_s)

    def hid_step(j, carry):
        cols = pl.ds(pl.multiple_of(j * HID_BLOCK, HID_BLOCK), HID_BLOCK)
        v = v_s[...]
        dz = dz_s[...]
        a = (dot(v, w_c1[:, cols]) + b_c1[:, cols]).astype(BF16)
        q32, slope = gelu_parts(a.astype(F32))
        q = q32.astype(BF16)
        dq = dot_nt(dz, w_c2[cols, :]).astype(BF16)
        da = (dq.astype(F32) * slope).astype(BF16)
        acc_s[...] += dot(q, w_c2[cols, :])
        dv_s[...] += dot_nt(da, w_c1[:, cols])
        g_c1[:, cols] += dot(vt_s[...], da)
        g_c2[cols, :] += dot(q.T, dz)
        return carry

    lax.fori_loop(0, hid // HID_BLOCK, hid_step, 0)

    for k in range(4):
        def ln2_back(i, carry, k=k):
            r = pl.multiple_of(i * ROW_BLOCK, 16)
            src = pl.ds(k * rows + r, ROW_BLOCK)
            x1 = x1_s[src, :].astype(F32)
            z_refs[k][0, pl.ds(r, ROW_BLOCK), :] = (x1 + (acc_s[src, :] + b_c2[...])).astype(BF16)
            dln = norm_grad(x1, dv_s[src, :].astype(BF16).astype(F32), ln2_s[...])
            v_s[src, :] = (dz_s[src, :].astype(F32) + dln.astype(F32)).astype(BF16)
            return carry

        lax.fori_loop(0, per_block, ln2_back, 0, unroll=True)

    g_t2[...] += dot_nt(g_s[...], v_s[...])
    for n in range(chans // COL_BLOCK):
        cols = slice(n * COL_BLOCK, (n + 1) * COL_BLOCK)
        dg = dot(w_t2[...], v_s[:, cols]).astype(BF16)
        dh = (dg.astype(F32) * gelu_slope(h_s[:, cols].astype(F32))).astype(BF16)
        g_s[:, cols] = dh
        dv_s[:, cols] = dot(w_t1[...], dh)
    g_t1[...] += dot_nt(u_s[...], g_s[...])

    for k in range(4):
        def ln1_back(i, carry, k=k):
            r = pl.multiple_of(i * ROW_BLOCK, 16)
            src = pl.ds(k * rows + r, ROW_BLOCK)
            x = x_refs[k][0, pl.ds(r, ROW_BLOCK), :].astype(F32)
            dln = norm_grad(x, dv_s[src, :].astype(BF16).astype(F32), ln1_s[...])
            dx_refs[k][0, pl.ds(r, ROW_BLOCK), :] = (v_s[src, :].astype(F32) + dln.astype(F32)).astype(BF16)
            return carry

        lax.fori_loop(0, per_block, ln1_back, 0, unroll=True)

    @pl.when(step == pl.num_programs(0) - 1)
    def _():
        copies = [pltpu.make_async_copy(acc, dst, sem.at[i])
                  for i, (acc, dst) in enumerate(zip(accs, acc_out))]
        for cp in copies:
            cp.start()
        for cp in copies:
            cp.wait()


def layer_call(xs, dzs, params, accs):
    images, rows, chans = xs[0].shape
    w_t1, w_c1 = params[8], params[12]
    total_rows, tok_hid = w_t1.shape
    hid = w_c1.shape[1]
    first = accs is None
    block = pl.BlockSpec((1, rows, chans), lambda i: (i, 0, 0))
    whole = pl.BlockSpec(memory_space=pltpu.VMEM)
    anywhere = pl.BlockSpec(memory_space=pl.ANY)
    acc_shapes = [(total_rows, tok_hid), (tok_hid, total_rows), (chans, hid), (hid, chans)]
    act = jax.ShapeDtypeStruct((images, rows, chans), BF16)
    out_shape = [act] * 8 + [jax.ShapeDtypeStruct(s, F32) for s in acc_shapes]
    n_in = 8 + len(params)
    acc_args = () if first else tuple(accs)
    flops = images * (12 * total_rows * chans * hid + 12 * total_rows * chans * tok_hid)
    return pl.pallas_call(
        functools.partial(layer_kernel, first),
        grid=(images,),
        in_specs=[block] * 8 + [whole] * len(params) + [anywhere] * len(acc_args),
        out_specs=[block] * 8 + [anywhere] * 4,
        out_shape=out_shape,
        scratch_shapes=[
            pltpu.VMEM(acc_shapes[2], F32), pltpu.VMEM(acc_shapes[3], F32),
            pltpu.VMEM(acc_shapes[0], F32), pltpu.VMEM(acc_shapes[1], F32),
            pltpu.VMEM((total_rows, chans), BF16), pltpu.VMEM((total_rows, chans), BF16),
            pltpu.VMEM((chans, total_rows), BF16), pltpu.VMEM((total_rows, chans), BF16),
            pltpu.VMEM((tok_hid, chans), BF16), pltpu.VMEM((tok_hid, chans), BF16),
            pltpu.VMEM((total_rows, chans), BF16),
            pltpu.VMEM((total_rows, chans), F32), pltpu.VMEM((total_rows, chans), F32),
            pltpu.SemaphoreType.DMA((4,)),
        ],
        input_output_aliases={} if first else {n_in + i: 8 + i for i in range(4)},
        compiler_params=pltpu.CompilerParams(
            dimension_semantics=("arbitrary",), vmem_limit_bytes=66_000_000),
        cost_estimate=pl.CostEstimate(flops=flops, bytes_accessed=60_000_000, transcendentals=0),
    )(*xs, *dzs, *params, *acc_args)


def solution(mesh):
    act_spec = P("data", "seq", None)
    part_spec = P("data", None)
    spec_in = (act_spec, act_spec) + (P(),) * 12
    spec_out = (act_spec, act_spec, part_spec, part_spec, part_spec, part_spec)
    ranks = mesh.shape["seq"]

    def hop(val, dist):
        return lax.ppermute(val, "seq", [(i, i ^ dist) for i in range(ranks)])

    def device_body(act_loc, grad_loc, ln1_scale, ln1_shift, w_tok1, b_tok1, w_tok2, b_tok2,
                    ln2_scale, ln2_shift, w_chan1, b_chan1, w_chan2, b_chan2):
        me = lax.axis_index("seq")
        core = me % 2
        images, rows, _ = act_loc.shape
        own = images // ranks

        def permute_blocks(arr, axis):
            parts = [lax.dynamic_slice_in_dim(arr, (me ^ d) * rows, rows, axis) for d in range(ranks)]
            return jnp.concatenate(parts, axis)

        w_t1 = permute_blocks(w_tok1, 0)
        w_t2 = permute_blocks(w_tok2, 1)
        b_t2 = permute_blocks(b_tok2, 0)
        params = (ln1_scale[None], ln1_shift[None], ln2_scale[None], ln2_shift[None], b_chan1[None], b_chan2[None],
                  b_tok1[:, None], b_t2[:, None], w_t1, w_t1.T, w_t2, w_t2.T,
                  w_chan1, w_chan2)

        def fetch(arr, start, size):
            blocks = []
            for d in range(ranks):
                piece = lax.dynamic_slice_in_dim(arr, (me ^ d) * own + start, size, 0)
                blocks.append(piece if d == 0 else hop(piece, d))
            return blocks

        starts = [sum(CHUNK_SIZES[:c]) for c in range(len(CHUNK_SIZES))]
        ins = [(fetch(act_loc, s, n), fetch(grad_loc, s, n))
               for s, n in zip(starts, CHUNK_SIZES)]
        act_out = jnp.zeros_like(act_loc)
        grad_in = jnp.zeros_like(act_loc)
        accs = None
        for c, offset in enumerate(starts):
            outs = layer_call(ins[c][0], ins[c][1], params, accs)
            accs = outs[8:]
            for d in range(ranks):
                z, dx = outs[d], outs[4 + d]
                if d:
                    z, dx = hop(z, d), hop(dx, d)
                start = (me ^ d) * own + offset
                act_out = lax.dynamic_update_slice_in_dim(act_out, z, start, 0)
                grad_in = lax.dynamic_update_slice_in_dim(grad_in, dx, start, 0)

        def group_sum(part, pieces):
            half = part.shape[0] // 2
            size = half // pieces
            out = jnp.zeros_like(part)
            for p in range(pieces):
                mine_at, other_at = core * half + p * size, (1 - core) * half + p * size
                mine = lax.dynamic_slice_in_dim(part, mine_at, size, 0)
                other = lax.dynamic_slice_in_dim(part, other_at, size, 0)
                pair = mine + hop(other, 1)
                full = pair + hop(pair, 2)
                peer = hop(full, 1)
                out = lax.dynamic_update_slice_in_dim(out, full, mine_at, 0)
                out = lax.dynamic_update_slice_in_dim(out, peer, other_at, 0)
            return out

        g_c1 = group_sum(accs[2], PIECES)
        g_c2 = group_sum(accs[3], PIECES)
        g_t1 = group_sum(permute_blocks(accs[0], 0), 1)
        g_t2 = group_sum(permute_blocks(accs[1], 1), 1)
        return act_out, grad_in, g_t1, g_t2, g_c1, g_c2

    return jax.shard_map(device_body, mesh=mesh, in_specs=spec_in, out_specs=spec_out, check_vma=False)
```

```python
import functools

import jax
import jax.numpy as jnp
from jax import lax
from jax.experimental import pallas as pl
from jax.experimental.pallas import tpu as pltpu
from jax.sharding import PartitionSpec as P


LN_EPS = 1e-6
GELU_C = 0.7978845608028654
GELU_K = 0.044715
F32 = jnp.float32
BF16 = jnp.bfloat16

CHUNK_SIZES = (2, 4, 6, 4)
PIECE_ROWS = 128
HID_BLOCK = 512
ROW_BLOCK = 48
COL_BLOCK = 256


def gelu_parts(pre):
    sq = pre * pre
    th = jnp.tanh(pre * (GELU_C + (GELU_C * GELU_K) * sq))
    one_plus = 1.0 + th
    inner_slope = pre * (0.5 * GELU_C + (1.5 * GELU_C * GELU_K) * sq)
    return (0.5 * pre) * one_plus, one_plus * (0.5 + inner_slope * (1.0 - th))


def gelu_value(pre):
    sq = pre * pre
    th = jnp.tanh(pre * (GELU_C + (GELU_C * GELU_K) * sq))
    return pre * (0.5 + 0.5 * th)


def gelu_slope(pre):
    return gelu_parts(pre)[1]


def dot(a, b):
    return jnp.dot(a, b, preferred_element_type=F32)


def dot_nt(a, b):
    return lax.dot_general(a, b, (((1,), (1,)), ((), ())), preferred_element_type=F32)


def layer_kernel(first, *refs):
    x_refs, dz_refs = refs[0:4], refs[4:8]
    (ln1_s, ln1_b, ln2_s, ln2_b, b_c1, b_c2, b_t1, b_t2, w_t1, w_t1t, w_t2, w_t2t,
     w_c1, w_c2) = refs[8:22]
    pos = 22
    if not first:
        tok_in, chan_in = refs[pos:pos + 2]
        pos += 2
    z_refs, dx_refs = refs[pos:pos + 4], refs[pos + 4:pos + 8]
    tok_out, chan_out = refs[pos + 8:pos + 10]
    (g_c1, g_c2, g_t1, g_t2, u_s, v_s, vt_s, dz_s, h_s, g_s, x1_s, dv_s, acc_s, dzt_s, stat_s, sem) = refs[pos + 10:]
    accs = (g_t1, g_t2, g_c1, g_c2)
    step = pl.program_id(0)
    rows = x_refs[0].shape[1]
    total_rows = 4 * rows
    chans = u_s.shape[1]
    hid = w_c1.shape[1]

    last_step = step == pl.num_programs(0) - 1

    def load_copies():
        srcs = (tok_in.at[0], tok_in.at[1], chan_in.at[0], chan_in.at[1])
        return [pltpu.make_async_copy(src, acc, sem.at[i]) for i, (src, acc) in enumerate(zip(srcs, accs))]

    def store_copy(i):
        dst = (tok_out, chan_out)[i // 2].at[i % 2]
        return pltpu.make_async_copy(accs[i], dst, sem.at[4 + i])

    @pl.when(step == 0)
    def _():
        if first:
            for acc in accs:
                acc[...] = jnp.zeros_like(acc)
        else:
            for cp in load_copies():
                cp.start()

    def widen(stat):
        return jnp.concatenate([stat] * (chans // 128), axis=1)

    def norm(val, scale, shift, mean_at, inv_at):
        mean = jnp.mean(val, axis=-1, keepdims=True)
        cen = val - mean
        var = jnp.mean(cen * cen, axis=-1, keepdims=True)
        inv = lax.rsqrt(var + LN_EPS)
        mean_at[...] = jnp.broadcast_to(mean, mean_at.shape)
        inv_at[...] = jnp.broadcast_to(inv, inv_at.shape)
        return (cen * inv * scale + shift).astype(BF16)

    def norm_grad(val, grad, scale, mean, inv):
        inv = widen(inv)
        hat = (val - widen(mean)) * inv
        gs = grad * scale
        m1 = jnp.mean(gs, axis=-1, keepdims=True)
        m2 = jnp.mean(gs * hat, axis=-1, keepdims=True)
        return (inv * (gs - m1 - hat * m2)).astype(BF16)

    per_block = rows // ROW_BLOCK

    for k in range(4):
        def ln1_step(i, carry, k=k):
            r = pl.multiple_of(i * ROW_BLOCK, 16)
            dst = pl.ds(k * rows + r, ROW_BLOCK)
            u_s[dst, :] = norm(x_refs[k][0, pl.ds(r, ROW_BLOCK), :].astype(F32), ln1_s[...], ln1_b[...],
                               stat_s.at[0, dst], stat_s.at[1, dst])
            dz_s[dst, :] = dz_refs[k][0, pl.ds(r, ROW_BLOCK), :]
            return carry

        lax.fori_loop(0, per_block, ln1_step, 0, unroll=True)

    for n in range(chans // COL_BLOCK):
        cols = slice(n * COL_BLOCK, (n + 1) * COL_BLOCK)
        h = (dot(w_t1t[...], u_s[:, cols]) + b_t1[...]).astype(BF16)
        h_s[:, cols] = h
        g = gelu_value(h.astype(F32)).astype(BF16)
        g_s[:, cols] = g
        t = (dot(w_t2t[...], g) + b_t2[...]).astype(BF16)
        for k in range(4):
            part = slice(k * rows, (k + 1) * rows)
            x1_s[part, cols] = (x_refs[k][0, :, cols].astype(F32) + t[part].astype(F32)).astype(BF16)

    def ln2_step(i, carry):
        r = pl.ds(pl.multiple_of(i * ROW_BLOCK, 16), ROW_BLOCK)
        x1 = x1_s[r, :].astype(F32)
        acc_s[r, :] = x1 + b_c2[...]
        v_s[r, :] = norm(x1, ln2_s[...], ln2_b[...], stat_s.at[2, r], stat_s.at[3, r])
        return carry

    lax.fori_loop(0, total_rows // ROW_BLOCK, ln2_step, 0, unroll=True)

    vt_s[...] = v_s[...].T
    dzt_s[...] = dz_s[...].T
    dv_s[...] = jnp.zeros_like(dv_s)

    if not first:
        @pl.when(step == 0)
        def _():
            for cp in load_copies():
                cp.wait()

    def hid_step(j, carry):
        cols = pl.ds(pl.multiple_of(j * HID_BLOCK, HID_BLOCK), HID_BLOCK)
        v = v_s[...]
        dz = dz_s[...]
        a = (dot(v, w_c1[:, cols]) + b_c1[:, cols]).astype(BF16)
        q32, slope = gelu_parts(a.astype(F32))
        q = q32.astype(BF16)
        dq = dot_nt(dz, w_c2[cols, :]).astype(BF16)
        da = (dq.astype(F32) * slope).astype(BF16)
        acc_s[...] += dot(q, w_c2[cols, :])
        dv_s[...] += dot_nt(da, w_c1[:, cols])
        g_c1[:, cols] += dot(vt_s[...], da)
        g_c2[:, cols] += dot(dzt_s[...], q)
        return carry

    lax.fori_loop(0, hid // HID_BLOCK, hid_step, 0)

    @pl.when(last_step)
    def _():
        store_copy(2).start()
        store_copy(3).start()

    for k in range(4):
        def ln2_back(i, carry, k=k):
            r = pl.multiple_of(i * ROW_BLOCK, 16)
            src = pl.ds(k * rows + r, ROW_BLOCK)
            x1 = x1_s[src, :].astype(F32)
            z_refs[k][0, pl.ds(r, ROW_BLOCK), :] = acc_s[src, :].astype(BF16)
            dln = norm_grad(x1, dv_s[src, :].astype(BF16).astype(F32), ln2_s[...], stat_s[2, src], stat_s[3, src])
            v_s[src, :] = (dz_s[src, :].astype(F32) + dln.astype(F32)).astype(BF16)
            return carry

        lax.fori_loop(0, per_block, ln2_back, 0, unroll=True)

    g_t2[...] += dot_nt(v_s[...], g_s[...])
    for n in range(chans // COL_BLOCK):
        cols = slice(n * COL_BLOCK, (n + 1) * COL_BLOCK)
        dg = dot(w_t2[...], v_s[:, cols]).astype(BF16)
        dh = (dg.astype(F32) * gelu_slope(h_s[:, cols].astype(F32))).astype(BF16)
        g_s[:, cols] = dh
        dv_s[:, cols] = dot(w_t1[...], dh)
    g_t1[...] += dot_nt(u_s[...], g_s[...])

    for k in range(4):
        def ln1_back(i, carry, k=k):
            r = pl.multiple_of(i * ROW_BLOCK, 16)
            src = pl.ds(k * rows + r, ROW_BLOCK)
            x = x_refs[k][0, pl.ds(r, ROW_BLOCK), :].astype(F32)
            dln = norm_grad(x, dv_s[src, :].astype(BF16).astype(F32), ln1_s[...], stat_s[0, src], stat_s[1, src])
            dx_refs[k][0, pl.ds(r, ROW_BLOCK), :] = (v_s[src, :].astype(F32) + dln.astype(F32)).astype(BF16)
            return carry

        lax.fori_loop(0, per_block, ln1_back, 0, unroll=True)

    @pl.when(last_step)
    def _():
        store_copy(0).start()
        store_copy(1).start()
        for i in range(4):
            store_copy(i).wait()


def layer_call(xs, dzs, params, accs):
    images, rows, chans = xs[0].shape
    w_t1, w_c1 = params[8], params[12]
    total_rows, tok_hid = w_t1.shape
    hid = w_c1.shape[1]
    first = accs is None
    block = pl.BlockSpec((1, rows, chans), lambda i: (i, 0, 0))
    whole = pl.BlockSpec(memory_space=pltpu.VMEM)
    anywhere = pl.BlockSpec(memory_space=pl.ANY)
    tok_shape, chan_shape = (total_rows, tok_hid), (chans, hid)
    act = jax.ShapeDtypeStruct((images, rows, chans), BF16)
    out_shape = [act] * 8 + [jax.ShapeDtypeStruct((2,) + tok_shape, F32), jax.ShapeDtypeStruct((2,) + chan_shape, F32)]
    n_in = 8 + len(params)
    acc_args = () if first else tuple(accs)
    flops = images * (12 * total_rows * chans * hid + 12 * total_rows * chans * tok_hid)
    return pl.pallas_call(
        functools.partial(layer_kernel, first),
        grid=(images,),
        in_specs=[block] * 8 + [whole] * len(params) + [anywhere] * len(acc_args),
        out_specs=[block] * 8 + [anywhere] * 2,
        out_shape=out_shape,
        scratch_shapes=[
            pltpu.VMEM(chan_shape, F32), pltpu.VMEM(chan_shape, F32),
            pltpu.VMEM(tok_shape, F32), pltpu.VMEM(tok_shape, F32),
            pltpu.VMEM((total_rows, chans), BF16), pltpu.VMEM((total_rows, chans), BF16),
            pltpu.VMEM((chans, total_rows), BF16), pltpu.VMEM((total_rows, chans), BF16),
            pltpu.VMEM((tok_hid, chans), BF16), pltpu.VMEM((tok_hid, chans), BF16),
            pltpu.VMEM((total_rows, chans), BF16),
            pltpu.VMEM((total_rows, chans), F32), pltpu.VMEM((total_rows, chans), F32),
            pltpu.VMEM((chans, total_rows), BF16),
            pltpu.VMEM((4, total_rows, 128), F32),
            pltpu.SemaphoreType.DMA((8,)),
        ],
        input_output_aliases={} if first else {n_in: 8, n_in + 1: 9},
        compiler_params=pltpu.CompilerParams(
            dimension_semantics=("arbitrary",), vmem_limit_bytes=66_000_000),
        cost_estimate=pl.CostEstimate(flops=flops, bytes_accessed=60_000_000, transcendentals=0),
    )(*xs, *dzs, *params, *acc_args)


def place_kernel(core_ref, full_ref, peer_ref, *refs):
    out1_ref, out2_ref = refs[-2:]
    is_first = core_ref[0] == 0
    full, peer = full_ref[...], peer_ref[...]
    out1_ref[...] = jnp.where(is_first, full, peer)
    out2_ref[...] = jnp.where(is_first, peer, full).T


def place_piece(core, full, peer, piece, bufs, chans):
    size, hid = full.shape
    width = 512
    part = pl.BlockSpec((size, width), lambda j, core_ref: (0, j))
    anywhere = pl.BlockSpec(memory_space=pl.ANY)
    bufs = () if bufs is None else tuple(bufs)
    return pl.pallas_call(
        place_kernel,
        grid_spec=pltpu.PrefetchScalarGridSpec(
            num_scalar_prefetch=1, grid=(hid // width,),
            in_specs=[part, part] + [anywhere] * len(bufs),
            out_specs=[pl.BlockSpec((size, width), lambda j, core_ref: (piece, j)),
                       pl.BlockSpec((width, size), lambda j, core_ref: (j, piece))]),
        out_shape=[jax.ShapeDtypeStruct((chans, hid), F32), jax.ShapeDtypeStruct((hid, chans), F32)],
        input_output_aliases={3 + i: i for i in range(len(bufs))},
        compiler_params=pltpu.CompilerParams(vmem_limit_bytes=16_000_000),
        cost_estimate=pl.CostEstimate(flops=0, bytes_accessed=4 * 4 * size * hid, transcendentals=0),
    )(core, full, peer, *bufs)


def solution(mesh):
    act_spec = P("data", "seq", None)
    part_spec = P("data", None)
    spec_in = (act_spec, act_spec) + (P(),) * 12
    spec_out = (act_spec, act_spec, part_spec, part_spec, part_spec, part_spec)
    ranks = mesh.shape["seq"]

    def hop(val, dist):
        return lax.ppermute(val, "seq", [(i, i ^ dist) for i in range(ranks)])

    def device_body(act_loc, grad_loc, ln1_scale, ln1_shift, w_tok1, b_tok1, w_tok2, b_tok2,
                    ln2_scale, ln2_shift, w_chan1, b_chan1, w_chan2, b_chan2):
        me = lax.axis_index("seq")
        core = me % 2
        images, rows, chans = act_loc.shape
        own = images // ranks

        def permute_blocks(arr, axis):
            parts = [lax.dynamic_slice_in_dim(arr, (me ^ d) * rows, rows, axis) for d in range(ranks)]
            return jnp.concatenate(parts, axis)

        w_t1 = permute_blocks(w_tok1, 0)
        w_t2 = permute_blocks(w_tok2, 1)
        b_t2 = permute_blocks(b_tok2, 0)
        params = (ln1_scale[None], ln1_shift[None], ln2_scale[None], ln2_shift[None], b_chan1[None], b_chan2[None],
                  b_tok1[:, None], b_t2[:, None], w_t1, w_t1.T, w_t2, w_t2.T,
                  w_chan1, w_chan2)

        def fetch(arr, start, size):
            blocks = []
            for d in range(ranks):
                piece = lax.dynamic_slice_in_dim(arr, (me ^ d) * own + start, size, 0)
                blocks.append(piece if d == 0 else hop(piece, d))
            return blocks

        starts = [sum(CHUNK_SIZES[:c]) for c in range(len(CHUNK_SIZES))]
        ins = [(fetch(act_loc, s, n), fetch(grad_loc, s, n))
               for s, n in zip(starts, CHUNK_SIZES)]
        accs = None
        back = []
        for c, offset in enumerate(starts):
            outs = layer_call(ins[c][0], ins[c][1], params, accs)
            accs = outs[8:]
            for d in range(ranks):
                z, dx = outs[d], outs[4 + d]
                if d:
                    z, dx = hop(z, d), hop(dx, d)
                back.append(((me ^ d) * own + offset, z, dx))

        tok, chan = accs
        tok = permute_blocks(tok, 1)

        def pair_sum(stack, at, size):
            width = stack.shape[2]
            mine = lax.dynamic_slice(stack, (core, at, 0), (1, size, width))[0]
            other = lax.dynamic_slice(stack, (1 - core, at, 0), (1, size, width))[0]
            got = hop(other, 1)
            return mine + got

        pieces = chans // PIECE_ROWS
        pairs = [pair_sum(chan, p * PIECE_ROWS, PIECE_ROWS) for p in range(pieces)]
        tok_pair = pair_sum(tok, 0, tok.shape[1])

        blank = jnp.zeros((), BF16)
        blank, pairs, tok_pair = lax.optimization_barrier((blank, pairs, tok_pair))
        act_out = jnp.broadcast_to(blank, act_loc.shape)
        grad_in = jnp.broadcast_to(blank, act_loc.shape)
        for start, z, dx in back:
            act_out = lax.dynamic_update_slice_in_dim(act_out, z, start, 0)
            grad_in = lax.dynamic_update_slice_in_dim(grad_in, dx, start, 0)

        bufs = None
        for p, pair in enumerate(pairs):
            got = hop(pair, 2)
            full = pair + got
            peer = hop(full, 1)
            bufs = place_piece(core[None], full, peer, p, bufs, chans)
        g_c1, g_c2 = bufs
        full = tok_pair + hop(tok_pair, 2)
        peer = hop(full, 1)
        g_t1 = jnp.where(core == 0, full, peer)
        g_t2 = jnp.where(core == 0, peer, full).T
        return act_out, grad_in, g_t1, g_t2, g_c1, g_c2

    return jax.shard_map(device_body, mesh=mesh, in_specs=spec_in, out_specs=spec_out, check_vma=False)
```
